32 devices in a mesh: space: 16 (over z, x, core), chan: 2 (over y).
Axes of the slice: x: 2, y: 2, z: 4, core: 2. Of those that a mesh axis runs over, the one named last changes fastest.
Arguments:
- inputs: bfloat16 [64, 32, 64, 128], P('chan', 'space'), may hold values from -6 to 6
- grad_out: bfloat16 [64, 32, 64, 128], P('chan', 'space'), may hold values from -6 to 6
- filt: bfloat16 [27, 64, 64], P(None, 'chan'), may hold values from -0.15625 to 0.15625
Outputs:
- grad_inputs: bfloat16 [64, 32, 64, 128], P('chan', 'space')
- grad_filt: float32 [27, 64, 64], P(None, 'chan', 'space')
The draws below stay inside these ranges and needn't reach their ends.
All inputs are finite; a program needn't handle non-finite values.
Results may differ from the reference program's by a relative error of at most 0.0066.
Values may be sent and summed in bfloat16 or wider, within the bound.
A program may use at most 128 MiB of HBM per device.

```python
import jax
import jax.numpy as jnp
from jax import lax

C = 64
O = 64
H = 64
W = 128
D = 32


def strengthened(entries, key, source, target, shards_of, factor):
    def block_of(position):
        return (jnp.arange(entries.shape[position]) // (entries.shape[position] // shards_of)).reshape((-1,) + (1,) * (entries.ndim - 1 - position))

    near = jax.random.permutation(key, shards_of)[block_of(target)]
    second = (block_of(target) + shards_of // 2) % shards_of
    return jnp.where((block_of(source) == near) | (block_of(source) == second), factor * entries, entries)


def steps_of(own_key, shape, cuts, low, largest):
    loudness, own = 1.0, jax.random.fold_in(own_key, 6)
    for dim, shards_of in cuts:
        heights = jnp.exp(jax.random.uniform(jax.random.fold_in(own, dim), (shards_of,), jnp.float32, low / len(cuts), largest / len(cuts)))
        loudness = loudness * jnp.repeat(heights, shape[dim] // shards_of).reshape([-1 if axis == dim else 1 for axis in range(len(shape))])
    return loudness


def noise(stream_key, extent, width, reach, pieces=(), kind=jnp.bfloat16):
    result = width * jax.random.normal(stream_key, extent, jnp.float32)
    if pieces:
        result = result * steps_of(stream_key, extent, pieces, -0.22, 0.18)
    return jnp.clip(result, -reach, reach).astype(kind)


def bell_draw_with(stream_key, dims, scale, bound, shards, heavy, dtype=jnp.bfloat16):
    array = scale * jax.random.normal(stream_key, dims, jnp.float32)
    if shards:
        array = array * steps_of(stream_key, dims, shards, -0.22, 0.18)
    return jnp.clip(strengthened(array, jax.random.fold_in(stream_key, 3), *heavy), -bound, bound).astype(dtype)


def setup_inputs(seed: int = 0) -> dict:
    splits = jax.random.split(jax.random.key(seed), 4)
    return {
        "inputs": noise(splits[0], (C, D, H, W), 1.0, 6.0, ((0, 2), (1, 16))),
        "grad_out": bell_draw_with(splits[1], (O, D, H, W), 1.0, 6.0, ((0, 2), (1, 16)), (1, 0, 16, 2.0)),
        "filt": noise(splits[2], (27, O, C), (27 * O) ** -0.5, 0.15625, ((1, 2),)),
    }


def reference(inputs, grad_out, filt):
    kernel = filt.astype(jnp.float32).reshape(3, 3, 3, O, C).transpose(3, 4, 0, 1, 2)

    def forward(volume, weights):
        return lax.conv_general_dilated(volume, weights, (1, 1, 1), [(1, 1), (1, 1), (1, 1)], dimension_numbers=('NCDHW', 'OIDHW', 'NCDHW'), precision=lax.Precision.HIGHEST)
    _, pullback = jax.vjp(forward, inputs.astype(jnp.float32)[None], kernel)
    grad_volume, grad_kernel = pullback(grad_out.astype(jnp.float32)[None])
    grad_inputs = grad_volume[0].astype(jnp.bfloat16)
    grad_filt = grad_kernel.transpose(2, 3, 4, 0, 1).reshape(27, O, C)
    return (grad_inputs, grad_filt)
```

```python
import functools

import jax
import jax.numpy as jnp
from jax import lax
from jax.experimental import pallas as pl
from jax.experimental.pallas import tpu as pltpu
from jax.sharding import PartitionSpec as P


def with_halo(x, sides, width):
    for axis, dim in sides:
        size, length = (lax.axis_size(axis), x.shape[dim])
        up = [(i, (i + 1) % size) for i in range(size - 1)]
        down = [(j, i) for i, j in up]
        last = lax.slice_in_dim(x, length - width, length, axis=dim)
        first = lax.slice_in_dim(x, 0, width, axis=dim)
        before = lax.ppermute(last, axis, up)
        after = lax.ppermute(first, axis, down)
        x = jnp.concatenate([before, x, after], axis=dim)
    return x


def columns(field):
    padded = jnp.pad(field, ((0, 0), (0, 0), (1, 1), (1, 1)))
    height = field.shape[2]
    row_len = field.shape[3]
    shifted = []
    for tap_row in range(3):
        for tap_col in range(3):
            shifted.append(
                padded[
                    :, :, 2 - tap_row : 2 - tap_row + height, 2 - tap_col : 2 - tap_col + row_len
                ]
            )
    return jnp.concatenate(shifted, axis=0)


def flat_window(field, first, planes):
    window = lax.slice_in_dim(field, first, first + planes, axis=1)
    return window.reshape(window.shape[0], -1)


def local(inputs, grad_out, filt):
    planes = inputs.shape[1]
    height = inputs.shape[2]
    row_len = inputs.shape[3]
    out_local = grad_out.shape[0]
    chan_total = filt.shape[2]
    tap_rows = 9 * out_local
    kernel = filt.reshape(3, tap_rows, chan_total)
    shifted_out = with_halo(grad_out, (("space", 1),), 1)
    stacked = columns(shifted_out)
    grad_left = [flat_window(stacked, 2 - depth_tap, planes) for depth_tap in range(3)]
    source_first = [0, 0, 0]
    segment = lax.all_gather(inputs, "chan", axis=0, tiled=True)
    blocks = []
    for depth_tap in range(3):
        right_side = flat_window(segment, source_first[depth_tap], planes)
        blocks.append(
            lax.dot_general(
                grad_left[depth_tap],
                right_side,
                (((1,), (1,)), ((), ())),
                preferred_element_type=jnp.float32,
            )
        )
    update = jnp.stack(blocks, 0)
    grad_filt = lax.psum_scatter(
        update.reshape(27, out_local, chan_total), "space", scatter_dimension=2, tiled=True
    )
    own_rows = chan_total // lax.axis_size("chan")
    total = None
    for depth_tap in range(3):
        product = lax.dot_general(
            kernel[depth_tap],
            grad_left[depth_tap],
            (((0,), (0,)), ((), ())),
            preferred_element_type=jnp.float32,
        )
        product = product.reshape(lax.axis_size("chan") * own_rows, planes, height, row_len)
        total = product if total is None else total + product
    summed = lax.psum_scatter(total, "chan", scatter_dimension=0, tiled=True)
    return (summed.astype(jnp.bfloat16), grad_filt)


ROWS = 16


def place(at, rel, size):
    return lax.rem(at + rel, size)


def body(
    n_space,
    n_chan,
    filt_ref,
    in_ref,
    out_hbm,
    gi_ref,
    gf_ref,
    raw,
    cols,
    source,
    held,
    total,
    weights,
    their_filt,
    sums,
    leave,
    land,
    own_sem,
    y_send,
    h_send,
    arrive,
    f_send,
    f_recv,
    s_send,
    s_recv,
):
    mine = in_ref.shape[0]
    height, width = in_ref.shape[2], in_ref.shape[3]
    chunks = height // ROWS
    group = 4 * mine
    s = lax.axis_index("space")
    k = lax.axis_index("chan")
    lane = lax.broadcasted_iota(jnp.int32, (mine, width), 1)

    def rows_of(c):
        return pl.ds(c * ROWS, ROWS)

    def y_copy(rel, plane, c):
        return pltpu.make_async_remote_copy(
            src_ref=out_hbm.at[:, plane, rows_of(c), :],
            dst_ref=raw.at[n_chan - rel, plane + 1, :, rows_of(c), :],
            send_sem=y_send.at[rel - 1, plane, c],
            recv_sem=arrive.at[n_chan - rel, plane + 1, c],
            device_id=(s, place(k, rel, n_chan)),
            device_id_type=pl.DeviceIdType.MESH,
        )

    def halo_copy(rel, side, c):
        if rel == 0:
            src = out_hbm.at[:, side, rows_of(c), :]
        else:
            src = raw.at[rel, side + 1, :, rows_of(c), :]
        land_plane = 3 if side == 0 else 0
        other = lax.max(s - 1, 0) if side == 0 else lax.min(s + 1, n_space - 1)
        return pltpu.make_async_remote_copy(
            src_ref=src,
            dst_ref=raw.at[rel, land_plane, :, rows_of(c), :],
            send_sem=h_send.at[rel, side, c],
            recv_sem=arrive.at[rel, land_plane, c],
            device_id=(other, k),
            device_id_type=pl.DeviceIdType.MESH,
        )

    def filt_copy(rel):
        return pltpu.make_async_remote_copy(
            src_ref=filt_ref.at[place(k, rel, n_chan)],
            dst_ref=their_filt.at[n_chan - rel],
            send_sem=f_send.at[rel - 1],
            recv_sem=f_recv.at[n_chan - rel - 1],
            device_id=(s, place(k, rel, n_chan)),
            device_id_type=pl.DeviceIdType.MESH,
        )

    def own_copy(plane):
        return pltpu.make_async_copy(
            out_hbm.at[:, plane], raw.at[0, plane + 1], own_sem.at[plane]
        )

    below, above = s > 0, s < n_space - 1

    def send_halo(rel, c):
        @pl.when(below)
        def _():
            halo_copy(rel, 0, c).start()

        @pl.when(above)
        def _():
            halo_copy(rel, 1, c).start()

    for rel in range(1, n_chan):
        filt_copy(rel).start()
    for c in range(chunks):
        for rel in range(1, n_chan):
            for plane in range(2):
                y_copy(rel, plane, c).start()
        send_halo(0, c)
    for plane in range(2):
        own_copy(plane).start()

    pad = jnp.zeros((source.shape[0], width), jnp.bfloat16)
    source[:, 0:width] = pad
    source[:, (height + 1) * width : (height + 2) * width] = pad
    pad = jnp.zeros((cols.shape[0], width), jnp.bfloat16)
    cols[:, 0:width] = pad
    cols[:, (height + 1) * width : (height + 2) * width] = pad

    def source_step(c, carry):
        first = pl.multiple_of(c * ROWS, ROWS)
        for plane in range(2):
            block = in_ref[:, plane, pl.ds(first, ROWS), :].astype(jnp.float32)
            held[...] = block.reshape(mine * ROWS, width)
            for h in range(ROWS):
                row = held[pl.ds(h, mine, stride=ROWS), :]
                left = jnp.where(lane > 0, pltpu.roll(row, 1, 1), 0.0)
                right = jnp.where(lane < width - 1, pltpu.roll(row, width - 1, 1), 0.0)
                at = pl.ds(pl.multiple_of((first + h + 1) * width, width), width)
                for e, value in enumerate((left, row, right)):
                    top = (2 * e + plane) * mine
                    source[top : top + mine, at] = value.astype(jnp.bfloat16)
        return carry

    lax.fori_loop(0, chunks, source_step, 0)

    def set_weights(rel, value):
        taps = value.astype(jnp.float32)
        moved = pltpu.roll(taps, mine, 1)
        for b in range(3):
            for e in range(3):
                at = (3 * b + e) * mine
                top = 2 * e * mine
                span = slice(rel * group, (rel + 1) * group)
                weights[b, top : top + mine, span] = taps[at : at + mine].astype(jnp.bfloat16)
                weights[b, top + mine : top + 2 * mine, span] = moved[at : at + mine].astype(
                    jnp.bfloat16
                )

    set_weights(0, filt_ref[k])
    for rel in range(1, n_chan):
        filt_copy(rel).wait()
    for rel in range(1, n_chan):
        set_weights(rel, their_filt[rel])

    def lay(rel, plane, c):
        block = raw[rel, plane, :, rows_of(c), :].astype(jnp.float32)
        held[...] = block.reshape(mine * ROWS, width)
        top = rel * group + plane * mine
        for h in range(ROWS):
            row = held[pl.ds(h, mine, stride=ROWS), :]
            at = (c * ROWS + h + 1) * width
            cols[top : top + mine, at : at + width] = row.astype(jnp.bfloat16)

    def lay_halo(rel, side, c):
        plane = 0 if side == 1 else 3
        there = below if side == 1 else above

        @pl.when(there)
        def _():
            halo_copy(rel, side, c).wait_recv()
            lay(rel, plane, c)

        @pl.when(jnp.logical_not(there))
        def _():
            top = rel * group + plane * mine
            first = (c * ROWS + 1) * width
            cols[top : top + mine, first : first + ROWS * width] = jnp.zeros(
                (mine, ROWS * width), jnp.bfloat16
            )

    def compute(c):
        first = (c * ROWS + 1) * width
        right = cols[:, first : first + ROWS * width]
        for b in range(3):
            begin = (c * ROWS + b) * width
            part = lax.dot_general(
                source[:, begin : begin + ROWS * width],
                right,
                (((1,), (1,)), ((), ())),
                preferred_element_type=jnp.float32,
            )
            if c == 0:
                total[b] = part
            else:
                total[b] += part

    def compute_inputs(c):
        low = 0 if c == 0 else c * ROWS - 2
        high = height if c == chunks - 1 else (c + 1) * ROWS - 2
        for h in range(low, high, 2):
            stack = jnp.concatenate(
                [cols[:, (h + 2 - b) * width : (h + 4 - b) * width] for b in range(3)], axis=0
            )
            taps = jnp.concatenate([weights[b] for b in range(3)], axis=1)
            got = jnp.dot(taps, stack, preferred_element_type=jnp.float32)
            for i in range(2):
                span = slice(i * width, (i + 1) * width)
                for plane in range(2):
                    at = plane * mine
                    lo = got[at : at + mine, span]
                    mid = got[2 * mine + at : 2 * mine + at + mine, span]
                    hi = got[4 * mine + at : 4 * mine + at + mine, span]
                    value = (
                        mid
                        + jnp.where(lane < width - 1, pltpu.roll(lo, width - 1, 1), 0.0)
                        + jnp.where(lane > 0, pltpu.roll(hi, 1, 1), 0.0)
                    )
                    sums[plane, pl.ds(h + i, mine, stride=height), :] = value

    for plane in range(2):
        own_copy(plane).wait()

    def step(c):
        for rel in range(n_chan):
            for side in range(2):
                lay_halo(rel, side, c)
        compute(c)
        if c < chunks - 1:
            compute_inputs(c)

    for c in range(chunks):
        for plane in range(2):
            lay(0, plane + 1, c)
        for rel in range(1, n_chan):
            for plane in range(2):
                y_copy(n_chan - rel, plane, c).wait_recv()
            send_halo(rel, c)
            for plane in range(2):
                lay(rel, plane + 1, c)
        if c:
            step(c - 1)
    step(chunks - 1)

    blocks = n_space // n_chan
    keep = mine // blocks
    leave[...] = jnp.zeros_like(leave)
    for rel in range(n_chan):
        span = slice(rel * group, (rel + 1) * group)
        for b in range(3):
            for e in range(3):
                top = 2 * e * mine
                share = total[b, top : top + mine, span] + pltpu.roll(
                    total[b, top + mine : top + 2 * mine, span], group - mine, 1
                )
                share = share.astype(jnp.bfloat16)
                at = (3 * b + e) * keep
                for j in range(blocks):
                    leave[rel, j, at : at + keep, :] = share[j * keep : (j + 1) * keep]

    def share_copy(rel, j):
        return pltpu.make_async_remote_copy(
            src_ref=leave.at[rel, j],
            dst_ref=land.at[s],
            send_sem=s_send.at[rel, j],
            recv_sem=s_recv.at[s],
            device_id=(k * blocks + j, place(k, rel, n_chan)),
            device_id_type=pl.DeviceIdType.MESH,
        )

    def each_share(act, own):
        for rel in range(n_chan):
            for turn in range(blocks):
                j = lax.rem(turn + s, blocks)
                if rel == 0:
                    here = k * blocks + j == s

                    @pl.when(jnp.logical_not(here))
                    def _():
                        act(share_copy(rel, j))

                    @pl.when(here)
                    def _():
                        if own:
                            pltpu.make_async_copy(
                                leave.at[rel, j], land.at[s], s_recv.at[s]
                            ).start()

                else:
                    act(share_copy(rel, j))

    each_share(lambda d: d.start(), True)
    compute_inputs(chunks - 1)
    for plane in range(2):
        gi_ref[:, plane] = sums[plane].reshape(mine, height, width).astype(jnp.bfloat16)

    for i in range(n_space):
        pltpu.make_async_copy(land.at[i], land.at[i], s_recv.at[i]).wait()
    result = land[0].astype(jnp.float32)
    for i in range(1, n_space):
        result += land[i].astype(jnp.float32)
    gf_ref[...] = result

    each_share(lambda d: d.wait_send(), False)
    for c in range(chunks):
        for rel in range(1, n_chan):
            for plane in range(2):
                y_copy(rel, plane, c).wait_send()
        for rel in range(n_chan):

            @pl.when(below)
            def _():
                halo_copy(rel, 0, c).wait_send()

            @pl.when(above)
            def _():
                halo_copy(rel, 1, c).wait_send()


def fused(n_space, n_chan, inputs, grad_out, filt):
    mine, planes, height, width = inputs.shape
    keep = filt.shape[2] // n_space
    blocks = n_space // n_chan
    taps = filt.reshape(3, 3, 3, mine, n_chan, mine)[::-1].transpose(4, 1, 2, 5, 0, 3)
    taps = taps.reshape(n_chan, 9 * mine, 3 * mine)
    taps = jnp.pad(taps, ((0, 0), (0, 0), (0, mine)))
    share_rows = -(-9 * keep // 16) * 16
    chunks = height // ROWS
    group = 4 * mine
    dma = pltpu.SemaphoreType.DMA
    vmem = pl.BlockSpec(memory_space=pltpu.VMEM)
    grad_inputs, share = pl.pallas_call(
        functools.partial(body, n_space, n_chan),
        out_shape=(
            jax.ShapeDtypeStruct(inputs.shape, jnp.bfloat16),
            jax.ShapeDtypeStruct((share_rows, group), jnp.float32),
        ),
        in_specs=[vmem, vmem, pl.BlockSpec(memory_space=pl.ANY)],
        out_specs=(vmem, vmem),
        scratch_shapes=[
            pltpu.VMEM((n_chan, 4, mine, height, width), jnp.bfloat16),
            pltpu.VMEM((n_chan * group, (height + 2) * width), jnp.bfloat16),
            pltpu.VMEM((6 * mine, (height + 2) * width), jnp.bfloat16),
            pltpu.VMEM((mine * ROWS, width), jnp.float32),
            pltpu.VMEM((3, 6 * mine, n_chan * group), jnp.float32),
            pltpu.VMEM((3, 6 * mine, n_chan * group), jnp.bfloat16),
            pltpu.VMEM((n_chan, 9 * mine, group), jnp.bfloat16),
            pltpu.VMEM((2, mine * height, width), jnp.float32),
            pltpu.VMEM((n_chan, blocks, share_rows, group), jnp.bfloat16),
            pltpu.VMEM((n_space, share_rows, group), jnp.bfloat16),
            dma((2,)),
            dma((n_chan - 1, 2, chunks)),
            dma((n_chan, 2, chunks)),
            dma((n_chan, 4, chunks)),
            dma((n_chan - 1,)),
            dma((n_chan - 1,)),
            dma((n_chan, blocks)),
            dma((n_space,)),
        ],
        compiler_params=pltpu.CompilerParams(has_side_effects=True, vmem_limit_bytes=56 << 20),
    )(taps, inputs, grad_out)
    share = share[: 9 * keep].reshape(9, keep, 4, mine)[:, :, 2::-1]
    return grad_inputs, share.transpose(2, 0, 3, 1).reshape(27, mine, keep)


def solution(mesh):
    n_space, n_chan = mesh.shape["space"], mesh.shape["chan"]

    def run(inputs, grad_out, filt):
        mine, planes, height, width = inputs.shape
        fits = (
            planes == 2
            and n_chan > 1
            and width == 128
            and 4 * mine == width
            and grad_out.shape[0] == mine
            and filt.shape[2] == n_chan * mine
            and height % ROWS == 0
            and n_space % n_chan == 0
            and filt.shape[2] % n_space == 0
        )
        if fits:
            return fused(n_space, n_chan, inputs, grad_out, filt)
        return local(inputs, grad_out, filt)

    return jax.shard_map(
        run,
        mesh=mesh,
        in_specs=(
            P("chan", "space", None, None),
            P("chan", "space", None, None),
            P(None, "chan", None),
        ),
        out_specs=(P("chan", "space", None, None), P(None, "chan", "space")),
        check_vma=False,
    )
```

```python
import functools

import jax
import jax.numpy as jnp
from jax import lax
from jax.experimental import pallas as pl
from jax.experimental.pallas import tpu as pltpu
from jax.sharding import PartitionSpec as P


def with_halo(x, sides, width):
    for axis, dim in sides:
        size, length = (lax.axis_size(axis), x.shape[dim])
        up = [(i, (i + 1) % size) for i in range(size - 1)]
        down = [(j, i) for i, j in up]
        last = lax.slice_in_dim(x, length - width, length, axis=dim)
        first = lax.slice_in_dim(x, 0, width, axis=dim)
        before = lax.ppermute(last, axis, up)
        after = lax.ppermute(first, axis, down)
        x = jnp.concatenate([before, x, after], axis=dim)
    return x


def columns(field):
    padded = jnp.pad(field, ((0, 0), (0, 0), (1, 1), (1, 1)))
    height = field.shape[2]
    row_len = field.shape[3]
    shifted = []
    for tap_row in range(3):
        for tap_col in range(3):
            shifted.append(
                padded[
                    :, :, 2 - tap_row : 2 - tap_row + height, 2 - tap_col : 2 - tap_col + row_len
                ]
            )
    return jnp.concatenate(shifted, axis=0)


def flat_window(field, first, planes):
    window = lax.slice_in_dim(field, first, first + planes, axis=1)
    return window.reshape(window.shape[0], -1)


def local(inputs, grad_out, filt):
    planes = inputs.shape[1]
    height = inputs.shape[2]
    row_len = inputs.shape[3]
    out_local = grad_out.shape[0]
    chan_total = filt.shape[2]
    tap_rows = 9 * out_local
    kernel = filt.reshape(3, tap_rows, chan_total)
    shifted_out = with_halo(grad_out, (("space", 1),), 1)
    stacked = columns(shifted_out)
    grad_left = [flat_window(stacked, 2 - depth_tap, planes) for depth_tap in range(3)]
    source_first = [0, 0, 0]
    segment = lax.all_gather(inputs, "chan", axis=0, tiled=True)
    blocks = []
    for depth_tap in range(3):
        right_side = flat_window(segment, source_first[depth_tap], planes)
        blocks.append(
            lax.dot_general(
                grad_left[depth_tap],
                right_side,
                (((1,), (1,)), ((), ())),
                preferred_element_type=jnp.float32,
            )
        )
    update = jnp.stack(blocks, 0)
    grad_filt = lax.psum_scatter(
        update.reshape(27, out_local, chan_total), "space", scatter_dimension=2, tiled=True
    )
    own_rows = chan_total // lax.axis_size("chan")
    total = None
    for depth_tap in range(3):
        product = lax.dot_general(
            kernel[depth_tap],
            grad_left[depth_tap],
            (((0,), (0,)), ((), ())),
            preferred_element_type=jnp.float32,
        )
        product = product.reshape(lax.axis_size("chan") * own_rows, planes, height, row_len)
        total = product if total is None else total + product
    summed = lax.psum_scatter(total, "chan", scatter_dimension=0, tiled=True)
    return (summed.astype(jnp.bfloat16), grad_filt)


ROWS = 16


def place(at, rel, size):
    return lax.rem(at + rel, size)


def body(
    n_space,
    n_chan,
    filt_ref,
    in_hbm,
    out_hbm,
    gi_ref,
    gf_ref,
    raw,
    cols,
    source,
    held,
    total,
    weights,
    in_ref,
    my_filt,
    their_filt,
    sums,
    leave,
    land,
    own_sem,
    in_sem,
    y_send,
    h_send,
    arrive,
    f_send,
    f_recv,
    s_send,
    s_recv,
):
    mine = in_ref.shape[0]
    height, width = in_ref.shape[2], in_ref.shape[3]
    chunks = height // ROWS
    group = 4 * mine
    s = lax.axis_index("space")
    k = lax.axis_index("chan")
    edge = lax.rem(s, 2)
    inner = 1 - edge
    lane = lax.broadcasted_iota(jnp.int32, (mine, width), 1)

    def rows_of(c):
        return pl.ds(c * ROWS, ROWS)

    def y_copy(rel, plane, c):
        return pltpu.make_async_remote_copy(
            src_ref=out_hbm.at[:, plane, rows_of(c), :],
            dst_ref=raw.at[n_chan - rel, plane + 1, :, rows_of(c), :],
            send_sem=y_send.at[rel - 1, plane, c],
            recv_sem=arrive.at[n_chan - rel, plane + 1, c],
            device_id=(s, place(k, rel, n_chan)),
            device_id_type=pl.DeviceIdType.MESH,
        )

    def halo_copy(rel, side, c):
        if rel == 0:
            src = out_hbm.at[:, side, rows_of(c), :]
        else:
            src = raw.at[rel, side + 1, :, rows_of(c), :]
        land_plane = 3 if side == 0 else 0
        other = lax.max(s - 1, 0) if side == 0 else lax.min(s + 1, n_space - 1)
        return pltpu.make_async_remote_copy(
            src_ref=src,
            dst_ref=raw.at[rel, land_plane, :, rows_of(c), :],
            send_sem=h_send.at[rel, side, c],
            recv_sem=arrive.at[rel, land_plane, c],
            device_id=(other, k),
            device_id_type=pl.DeviceIdType.MESH,
        )

    def filt_copy(rel):
        return pltpu.make_async_remote_copy(
            src_ref=my_filt.at[place(k, rel, n_chan)],
            dst_ref=their_filt.at[n_chan - rel],
            send_sem=f_send.at[rel - 1],
            recv_sem=f_recv.at[n_chan - rel - 1],
            device_id=(s, place(k, rel, n_chan)),
            device_id_type=pl.DeviceIdType.MESH,
        )

    def own_copy(plane):
        return pltpu.make_async_copy(
            out_hbm.at[:, plane], raw.at[0, plane + 1], own_sem.at[plane]
        )

    below, above = s > 0, s < n_space - 1

    def send_halo(rel, c):
        @pl.when(below)
        def _():
            halo_copy(rel, 0, c).start()

        @pl.when(above)
        def _():
            halo_copy(rel, 1, c).start()

    def start_y(plane, c):
        for rel in range(1, n_chan):
            y_copy(rel, plane, c).start()

    load = pltpu.make_async_copy(in_hbm, in_ref, in_sem.at[0])
    start_y(edge, 0)
    load.start()
    for plane in range(2):
        own_copy(plane).start()
    for c in range(chunks):
        send_halo(0, c)

    for b in range(3):
        for e in range(3):
            taps = [filt_ref[9 * (2 - p) + 3 * b + e].astype(jnp.float32) for p in range(3)]
            turned = jnp.concatenate(taps + [jnp.zeros_like(taps[0])], axis=0).T
            at = (3 * b + e) * mine
            for part in range(n_chan):
                my_filt[part, at : at + mine, :] = turned[
                    part * mine : (part + 1) * mine
                ].astype(jnp.bfloat16)
    for rel in range(1, n_chan):
        filt_copy(rel).start()
    for c in range(chunks):
        if c < chunks - 1:
            start_y(edge, c + 1)
        start_y(inner, c)

    pad = jnp.zeros((source.shape[0], width), jnp.bfloat16)
    source[:, 0:width] = pad
    source[:, (height + 1) * width : (height + 2) * width] = pad
    pad = jnp.zeros((cols.shape[0], width), jnp.bfloat16)
    cols[:, 0:width] = pad
    cols[:, (height + 1) * width : (height + 2) * width] = pad

    def source_step(c, carry):
        first = pl.multiple_of(c * ROWS, ROWS)
        for plane in range(2):
            block = in_ref[:, plane, pl.ds(first, ROWS), :].astype(jnp.float32)
            held[...] = block.reshape(mine * ROWS, width)
            for h in range(ROWS):
                row = held[pl.ds(h, mine, stride=ROWS), :]
                left = jnp.where(lane > 0, pltpu.roll(row, 1, 1), 0.0)
                right = jnp.where(lane < width - 1, pltpu.roll(row, width - 1, 1), 0.0)
                at = pl.ds(pl.multiple_of((first + h + 1) * width, width), width)
                for e, value in enumerate((left, row, right)):
                    top = (2 * e + plane) * mine
                    source[top : top + mine, at] = value.astype(jnp.bfloat16)
        return carry

    load.wait()
    lax.fori_loop(0, chunks, source_step, 0)

    def set_weights(rel, value):
        taps = value.astype(jnp.float32)
        moved = pltpu.roll(taps, mine, 1)
        for b in range(3):
            for e in range(3):
                at = (3 * b + e) * mine
                top = 2 * e * mine
                span = slice(rel * group, (rel + 1) * group)
                weights[b, top : top + mine, span] = taps[at : at + mine].astype(jnp.bfloat16)
                weights[b, top + mine : top + 2 * mine, span] = moved[at : at + mine].astype(
                    jnp.bfloat16
                )

    set_weights(0, my_filt[k])
    for rel in range(1, n_chan):
        filt_copy(rel).wait()
    for rel in range(1, n_chan):
        set_weights(rel, their_filt[rel])

    def lay(rel, plane, c):
        block = raw[rel, plane, :, rows_of(c), :].astype(jnp.float32)
        held[...] = block.reshape(mine * ROWS, width)
        top = rel * group + plane * mine
        for h in range(ROWS):
            row = held[pl.ds(h, mine, stride=ROWS), :]
            at = (c * ROWS + h + 1) * width
            cols[top : top + mine, at : at + width] = row.astype(jnp.bfloat16)

    def lay_halo(rel, side, c):
        plane = 0 if side == 1 else 3
        there = below if side == 1 else above

        @pl.when(there)
        def _():
            halo_copy(rel, side, c).wait_recv()
            lay(rel, plane, c)

        @pl.when(jnp.logical_not(there))
        def _():
            top = rel * group + plane * mine
            first = (c * ROWS + 1) * width
            cols[top : top + mine, first : first + ROWS * width] = jnp.zeros(
                (mine, ROWS * width), jnp.bfloat16
            )

    def compute(rel, c):
        first = (c * ROWS + 1) * width
        right = cols[rel * group : (rel + 1) * group, first : first + ROWS * width]
        for b in range(3):
            begin = (c * ROWS + b) * width
            part = lax.dot_general(
                source[:, begin : begin + ROWS * width],
                right,
                (((1,), (1,)), ((), ())),
                preferred_element_type=jnp.float32,
            )
            if c == 0:
                total[rel, b] = part
            else:
                total[rel, b] += part

    def compute_inputs(c):
        low = 0 if c == 0 else c * ROWS - 2
        high = height if c == chunks - 1 else (c + 1) * ROWS - 2
        for h in range(low, high, 2):
            stack = jnp.concatenate(
                [cols[:, (h + 2 - b) * width : (h + 4 - b) * width] for b in range(3)], axis=0
            )
            taps = jnp.concatenate([weights[b] for b in range(3)], axis=1)
            got = jnp.dot(taps, stack, preferred_element_type=jnp.float32)
            for i in range(2):
                span = slice(i * width, (i + 1) * width)
                for plane in range(2):
                    at = plane * mine
                    lo = got[at : at + mine, span]
                    mid = got[2 * mine + at : 2 * mine + at + mine, span]
                    hi = got[4 * mine + at : 4 * mine + at + mine, span]
                    value = (
                        mid
                        + jnp.where(lane < width - 1, pltpu.roll(lo, width - 1, 1), 0.0)
                        + jnp.where(lane > 0, pltpu.roll(hi, 1, 1), 0.0)
                    )
                    sums[plane, pl.ds(h + i, mine, stride=height), :] = value

    def round_rows(c):
        first = c * ROWS
        for plane in range(2):
            for i in range(mine):
                value = sums[plane, i * height + first : i * height + first + ROWS, :]
                gi_ref[i, plane, first : first + ROWS, :] = value.astype(jnp.bfloat16)

    def lay_own(c):
        for plane in range(2):
            lay(0, plane + 1, c)
        for side in range(2):
            lay_halo(0, side, c)
        compute(0, c)

    def finish(c):
        for rel in range(1, n_chan):
            for side in range(2):
                lay_halo(rel, side, c)
            compute(rel, c)

    def forward(plane, c):
        for rel in range(1, n_chan):
            y_copy(n_chan - rel, plane, c).wait_recv()

            @pl.when(jnp.logical_and(plane == 0, below))
            def _():
                halo_copy(rel, 0, c).start()

            @pl.when(jnp.logical_and(plane == 1, above))
            def _():
                halo_copy(rel, 1, c).start()

    blocks = n_space // n_chan
    keep = mine // blocks
    leave[...] = jnp.zeros_like(leave)

    def fill_share(rel):
        for b in range(3):
            for e in range(3):
                top = 2 * e * mine
                share = total[rel, b, top : top + mine, :] + pltpu.roll(
                    total[rel, b, top + mine : top + 2 * mine, :], group - mine, 1
                )
                share = share.astype(jnp.bfloat16)
                at = (3 * b + e) * keep
                for j in range(blocks):
                    leave[rel, j, at : at + keep, :] = share[j * keep : (j + 1) * keep]

    def share_copy(rel, j):
        return pltpu.make_async_remote_copy(
            src_ref=leave.at[rel, j],
            dst_ref=land.at[s],
            send_sem=s_send.at[rel, j],
            recv_sem=s_recv.at[s],
            device_id=(k * blocks + j, place(k, rel, n_chan)),
            device_id_type=pl.DeviceIdType.MESH,
        )

    def each_share(rel, act, own):
        for turn in range(blocks):
            j = lax.rem(turn + s, blocks)
            if rel == 0:
                here = k * blocks + j == s

                @pl.when(jnp.logical_not(here))
                def _():
                    act(share_copy(rel, j))

                if own:

                    @pl.when(here)
                    def _():
                        pltpu.make_async_copy(leave.at[rel, j], land.at[s], s_recv.at[s]).start()

            else:
                act(share_copy(rel, j))

    def send_share(rel):
        fill_share(rel)
        each_share(rel, lambda d: d.start(), True)

    for plane in range(2):
        own_copy(plane).wait()
    forward(edge, 0)
    for c in range(chunks):
        if c < chunks - 1:
            forward(edge, c + 1)
            lay_own(c)
        if c == chunks - 2:
            lay_own(chunks - 1)
            send_share(0)
        if c:
            finish(c - 1)
            compute_inputs(c - 1)
            if c > 1:
                round_rows(c - 2)
        forward(inner, c)
        for rel in range(1, n_chan):
            for plane in range(2):
                lay(rel, plane + 1, c)
    finish(chunks - 1)
    for rel in range(1, n_chan):
        send_share(rel)
    compute_inputs(chunks - 1)
    for c in range(max(chunks - 2, 0), chunks):
        round_rows(c)

    for i in range(n_space):
        pltpu.make_async_copy(land.at[i], land.at[i], s_recv.at[i]).wait()
    result = land[0].astype(jnp.float32)
    for i in range(1, n_space):
        result += land[i].astype(jnp.float32)
    gf_ref[...] = result

    for rel in range(n_chan):
        each_share(rel, lambda d: d.wait_send(), False)
    for c in range(chunks):
        for rel in range(1, n_chan):
            for plane in range(2):
                y_copy(rel, plane, c).wait_send()
        for rel in range(n_chan):

            @pl.when(below)
            def _():
                halo_copy(rel, 0, c).wait_send()

            @pl.when(above)
            def _():
                halo_copy(rel, 1, c).wait_send()


def fused(n_space, n_chan, inputs, grad_out, filt):
    mine, planes, height, width = inputs.shape
    keep = filt.shape[2] // n_space
    blocks = n_space // n_chan
    share_rows = -(-9 * keep // 16) * 16
    chunks = height // ROWS
    group = 4 * mine
    dma = pltpu.SemaphoreType.DMA
    vmem = pl.BlockSpec(memory_space=pltpu.VMEM)
    grad_inputs, share = pl.pallas_call(
        functools.partial(body, n_space, n_chan),
        out_shape=(
            jax.ShapeDtypeStruct(inputs.shape, jnp.bfloat16),
            jax.ShapeDtypeStruct((share_rows, group), jnp.float32),
        ),
        in_specs=[vmem, pl.BlockSpec(memory_space=pl.ANY), pl.BlockSpec(memory_space=pl.ANY)],
        out_specs=(vmem, vmem),
        scratch_shapes=[
            pltpu.VMEM((n_chan, 4, mine, height, width), jnp.bfloat16),
            pltpu.VMEM((n_chan * group, (height + 2) * width), jnp.bfloat16),
            pltpu.VMEM((6 * mine, (height + 2) * width), jnp.bfloat16),
            pltpu.VMEM((mine * ROWS, width), jnp.float32),
            pltpu.VMEM((n_chan, 3, 6 * mine, group), jnp.float32),
            pltpu.VMEM((3, 6 * mine, n_chan * group), jnp.bfloat16),
            pltpu.VMEM(inputs.shape, jnp.bfloat16),
            pltpu.VMEM((n_chan, 9 * mine, group), jnp.bfloat16),
            pltpu.VMEM((n_chan, 9 * mine, group), jnp.bfloat16),
            pltpu.VMEM((2, mine * height, width), jnp.float32),
            pltpu.VMEM((n_chan, blocks, share_rows, group), jnp.bfloat16),
            pltpu.VMEM((n_space, share_rows, group), jnp.bfloat16),
            dma((2,)),
            dma((1,)),
            dma((n_chan - 1, 2, chunks)),
            dma((n_chan, 2, chunks)),
            dma((n_chan, 4, chunks)),
            dma((n_chan - 1,)),
            dma((n_chan - 1,)),
            dma((n_chan, blocks)),
            dma((n_space,)),
        ],
        compiler_params=pltpu.CompilerParams(has_side_effects=True, vmem_limit_bytes=24 << 20),
    )(filt, inputs, grad_out)
    share = share[: 9 * keep].reshape(9, keep, 4, mine)[:, :, 2::-1]
    return grad_inputs, share.transpose(2, 0, 3, 1).reshape(27, mine, keep)


def solution(mesh):
    n_space, n_chan = mesh.shape["space"], mesh.shape["chan"]

    def run(inputs, grad_out, filt):
        mine, planes, height, width = inputs.shape
        fits = (
            planes == 2
            and n_chan > 1
            and width == 128
            and 4 * mine == width
            and grad_out.shape[0] == mine
            and filt.shape[2] == n_chan * mine
            and height % ROWS == 0
            and n_space % n_chan == 0
            and filt.shape[2] % n_space == 0
        )
        if fits:
            return fused(n_space, n_chan, inputs, grad_out, filt)
        return local(inputs, grad_out, filt)

    return jax.shard_map(
        run,
        mesh=mesh,
        in_specs=(
            P("chan", "space", None, None),
            P("chan", "space", None, None),
            P(None, "chan", None),
        ),
        out_specs=(P("chan", "space", None, None), P(None, "chan", "space")),
        check_vma=False,
    )
```

```python
import functools

import jax
import jax.numpy as jnp
from jax import lax
from jax.experimental import pallas as pl
from jax.experimental.pallas import tpu as pltpu
from jax.sharding import PartitionSpec as P


def with_halo(x, sides, width):
    for axis, dim in sides:
        size, length = (lax.axis_size(axis), x.shape[dim])
        up = [(i, (i + 1) % size) for i in range(size - 1)]
        down = [(j, i) for i, j in up]
        last = lax.slice_in_dim(x, length - width, length, axis=dim)
        first = lax.slice_in_dim(x, 0, width, axis=dim)
        before = lax.ppermute(last, axis, up)
        after = lax.ppermute(first, axis, down)
        x = jnp.concatenate([before, x, after], axis=dim)
    return x


def columns(field):
    padded = jnp.pad(field, ((0, 0), (0, 0), (1, 1), (1, 1)))
    height = field.shape[2]
    row_len = field.shape[3]
    shifted = []
    for tap_row in range(3):
        for tap_col in range(3):
            shifted.append(
                padded[
                    :, :, 2 - tap_row : 2 - tap_row + height, 2 - tap_col : 2 - tap_col + row_len
                ]
            )
    return jnp.concatenate(shifted, axis=0)


def flat_window(field, first, planes):
    window = lax.slice_in_dim(field, first, first + planes, axis=1)
    return window.reshape(window.shape[0], -1)


def local(inputs, grad_out, filt):
    planes = inputs.shape[1]
    height = inputs.shape[2]
    row_len = inputs.shape[3]
    out_local = grad_out.shape[0]
    chan_total = filt.shape[2]
    tap_rows = 9 * out_local
    kernel = filt.reshape(3, tap_rows, chan_total)
    shifted_out = with_halo(grad_out, (("space", 1),), 1)
    stacked = columns(shifted_out)
    grad_left = [flat_window(stacked, 2 - depth_tap, planes) for depth_tap in range(3)]
    source_first = [0, 0, 0]
    segment = lax.all_gather(inputs, "chan", axis=0, tiled=True)
    blocks = []
    for depth_tap in range(3):
        right_side = flat_window(segment, source_first[depth_tap], planes)
        blocks.append(
            lax.dot_general(
                grad_left[depth_tap],
                right_side,
                (((1,), (1,)), ((), ())),
                preferred_element_type=jnp.float32,
            )
        )
    update = jnp.stack(blocks, 0)
    grad_filt = lax.psum_scatter(
        update.reshape(27, out_local, chan_total), "space", scatter_dimension=2, tiled=True
    )
    own_rows = chan_total // lax.axis_size("chan")
    total = None
    for depth_tap in range(3):
        product = lax.dot_general(
            kernel[depth_tap],
            grad_left[depth_tap],
            (((0,), (0,)), ((), ())),
            preferred_element_type=jnp.float32,
        )
        product = product.reshape(lax.axis_size("chan") * own_rows, planes, height, row_len)
        total = product if total is None else total + product
    summed = lax.psum_scatter(total, "chan", scatter_dimension=0, tiled=True)
    return (summed.astype(jnp.bfloat16), grad_filt)


ROWS = 16


def place(at, rel, size):
    return lax.rem(at + rel, size)


def body(
    n_space,
    n_chan,
    filt_hbm,
    in_hbm,
    out_hbm,
    gi_ref,
    gf_ref,
    raw,
    cols,
    source,
    held,
    total,
    weights,
    in_ref,
    filt_ref,
    my_filt,
    their_filt,
    sums,
    leave,
    land,
    own_sem,
    in_sem,
    y_send,
    h_send,
    arrive,
    f_send,
    f_recv,
    s_send,
    s_recv,
    met,
):
    mine = in_ref.shape[0]
    height, width = in_ref.shape[2], in_ref.shape[3]
    chunks = height // ROWS
    group = 4 * mine
    s = lax.axis_index("space")
    k = lax.axis_index("chan")
    edge = lax.rem(s, 2)
    inner = 1 - edge
    lane = lax.broadcasted_iota(jnp.int32, (mine, width), 1)

    def partner(b):
        bit = 1 << b
        return s + bit - 2 * bit * lax.rem(s // bit, 2)

    def rows_of(c):
        return pl.ds(c * ROWS, ROWS)

    def y_copy(rel, plane, c):
        return pltpu.make_async_remote_copy(
            src_ref=out_hbm.at[:, plane, rows_of(c), :],
            dst_ref=raw.at[n_chan - rel, plane + 1, :, rows_of(c), :],
            send_sem=y_send.at[rel - 1, plane, c],
            recv_sem=arrive.at[n_chan - rel, plane + 1, c],
            device_id=(s, place(k, rel, n_chan)),
            device_id_type=pl.DeviceIdType.MESH,
        )

    def halo_copy(rel, side, c):
        if rel == 0:
            src = out_hbm.at[:, side, rows_of(c), :]
        else:
            src = raw.at[rel, side + 1, :, rows_of(c), :]
        land_plane = 3 if side == 0 else 0
        other = lax.max(s - 1, 0) if side == 0 else lax.min(s + 1, n_space - 1)
        return pltpu.make_async_remote_copy(
            src_ref=src,
            dst_ref=raw.at[rel, land_plane, :, rows_of(c), :],
            send_sem=h_send.at[rel, side, c],
            recv_sem=arrive.at[rel, land_plane, c],
            device_id=(other, k),
            device_id_type=pl.DeviceIdType.MESH,
        )

    def filt_copy(rel):
        return pltpu.make_async_remote_copy(
            src_ref=my_filt.at[place(k, rel, n_chan)],
            dst_ref=their_filt.at[n_chan - rel],
            send_sem=f_send.at[rel - 1],
            recv_sem=f_recv.at[n_chan - rel - 1],
            device_id=(s, place(k, rel, n_chan)),
            device_id_type=pl.DeviceIdType.MESH,
        )

    def own_copy(plane):
        return pltpu.make_async_copy(
            out_hbm.at[:, plane], raw.at[0, plane + 1], own_sem.at[plane]
        )

    below, above = s > 0, s < n_space - 1

    def send_halo(rel, c):
        @pl.when(below)
        def _():
            halo_copy(rel, 0, c).start()

        @pl.when(above)
        def _():
            halo_copy(rel, 1, c).start()

    rounds = n_space.bit_length() - 1
    mesh_id = pl.DeviceIdType.MESH
    barrier = pltpu.get_barrier_semaphore()
    for b in range(rounds):
        pl.semaphore_signal(
            barrier, inc=1, device_id=(partner(b), k), device_id_type=mesh_id
        )
    for rel in range(1, n_chan):
        pl.semaphore_signal(
            barrier, inc=1, device_id=(s, place(k, rel, n_chan)), device_id_type=mesh_id
        )

    @pl.when(jnp.logical_and(edge == 0, below))
    def _():
        pl.semaphore_signal(barrier, inc=1, device_id=(s - 1, k), device_id_type=mesh_id)

    @pl.when(jnp.logical_and(edge == 1, above))
    def _():
        pl.semaphore_signal(barrier, inc=1, device_id=(s + 1, k), device_id_type=mesh_id)

    beside = jnp.where(edge == 0, s > 0, s < n_space - 1).astype(jnp.int32)
    pl.semaphore_wait(barrier, rounds + n_chan - 1 + beside)

    def advance(i):
        if i > 0:
            pl.semaphore_wait(met.at[i - 1], 1 if i <= rounds else n_chan - 1)
        if i < rounds:
            pl.semaphore_signal(
                met.at[i], inc=1, device_id=(partner(i), k), device_id_type=mesh_id
            )
        elif i == rounds:
            for rel in range(1, n_chan):
                pl.semaphore_signal(
                    met.at[i],
                    inc=1,
                    device_id=(s, place(k, rel, n_chan)),
                    device_id_type=mesh_id,
                )

    def start_y(plane, c):
        for rel in range(1, n_chan):
            y_copy(rel, plane, c).start()

    load = pltpu.make_async_copy(in_hbm, in_ref, in_sem.at[0])
    start_y(edge, 0)
    load_filt = pltpu.make_async_copy(filt_hbm, filt_ref, in_sem.at[1])
    load_filt.start()
    load.start()
    for plane in range(2):
        own_copy(plane).start()
    for c in range(chunks):
        send_halo(0, c)

    advance(0)
    load_filt.wait()
    for b in range(3):
        for e in range(3):
            taps = [filt_ref[9 * (2 - p) + 3 * b + e].astype(jnp.float32) for p in range(3)]
            turned = jnp.concatenate(taps + [jnp.zeros_like(taps[0])], axis=0).T
            at = (3 * b + e) * mine
            for part in range(n_chan):
                my_filt[part, at : at + mine, :] = turned[
                    part * mine : (part + 1) * mine
                ].astype(jnp.bfloat16)
    for rel in range(1, n_chan):
        filt_copy(rel).start()
    for c in range(chunks):
        if c < chunks - 1:
            start_y(edge, c + 1)
        start_y(inner, c)
    advance(1)

    pad = jnp.zeros((source.shape[0], width), jnp.bfloat16)
    source[:, 0:width] = pad
    source[:, (height + 1) * width : (height + 2) * width] = pad
    pad = jnp.zeros((cols.shape[0], width), jnp.bfloat16)
    cols[:, 0:width] = pad
    cols[:, (height + 1) * width : (height + 2) * width] = pad

    def source_step(c, carry):
        first = pl.multiple_of(c * ROWS, ROWS)
        for plane in range(2):
            block = in_ref[:, plane, pl.ds(first, ROWS), :].astype(jnp.float32)
            held[...] = block.reshape(mine * ROWS, width)
            for h in range(ROWS):
                row = held[pl.ds(h, mine, stride=ROWS), :]
                left = jnp.where(lane > 0, pltpu.roll(row, 1, 1), 0.0)
                right = jnp.where(lane < width - 1, pltpu.roll(row, width - 1, 1), 0.0)
                at = pl.ds(pl.multiple_of((first + h + 1) * width, width), width)
                for e, value in enumerate((left, row, right)):
                    top = (2 * e + plane) * mine
                    source[top : top + mine, at] = value.astype(jnp.bfloat16)
        return carry

    load.wait()
    lax.fori_loop(0, chunks, source_step, 0)
    advance(2)

    def set_weights(rel, value):
        taps = value.astype(jnp.float32)
        moved = pltpu.roll(taps, mine, 1)
        for b in range(3):
            for e in range(3):
                at = (3 * b + e) * mine
                top = 2 * e * mine
                span = slice(rel * group, (rel + 1) * group)
                weights[b, top : top + mine, span] = taps[at : at + mine].astype(jnp.bfloat16)
                weights[b, top + mine : top + 2 * mine, span] = moved[at : at + mine].astype(
                    jnp.bfloat16
                )

    set_weights(0, my_filt[k])
    for rel in range(1, n_chan):
        filt_copy(rel).wait()
    for rel in range(1, n_chan):
        set_weights(rel, their_filt[rel])

    advance(3)

    def lay(rel, plane, c):
        block = raw[rel, plane, :, rows_of(c), :].astype(jnp.float32)
        held[...] = block.reshape(mine * ROWS, width)
        top = rel * group + plane * mine
        for h in range(ROWS):
            row = held[pl.ds(h, mine, stride=ROWS), :]
            at = (c * ROWS + h + 1) * width
            cols[top : top + mine, at : at + width] = row.astype(jnp.bfloat16)

    def lay_halo(rel, side, c):
        plane = 0 if side == 1 else 3
        there = below if side == 1 else above

        @pl.when(there)
        def _():
            halo_copy(rel, side, c).wait_recv()
            lay(rel, plane, c)

        @pl.when(jnp.logical_not(there))
        def _():
            top = rel * group + plane * mine
            first = (c * ROWS + 1) * width
            cols[top : top + mine, first : first + ROWS * width] = jnp.zeros(
                (mine, ROWS * width), jnp.bfloat16
            )

    def compute(rel, c):
        first = (c * ROWS + 1) * width
        right = cols[rel * group : (rel + 1) * group, first : first + ROWS * width]
        for b in range(3):
            begin = (c * ROWS + b) * width
            part = lax.dot_general(
                source[:, begin : begin + ROWS * width],
                right,
                (((1,), (1,)), ((), ())),
                preferred_element_type=jnp.float32,
            )
            if c == 0:
                total[rel, b] = part
            else:
                total[rel, b] += part

    def compute_inputs(c):
        low = 0 if c == 0 else c * ROWS - 2
        high = height if c == chunks - 1 else (c + 1) * ROWS - 2
        for h in range(low, high, 2):
            stack = jnp.concatenate(
                [cols[:, (h + 2 - b) * width : (h + 4 - b) * width] for b in range(3)], axis=0
            )
            taps = jnp.concatenate([weights[b] for b in range(3)], axis=1)
            got = jnp.dot(taps, stack, preferred_element_type=jnp.float32)
            for i in range(2):
                span = slice(i * width, (i + 1) * width)
                for plane in range(2):
                    at = plane * mine
                    lo = got[at : at + mine, span]
                    mid = got[2 * mine + at : 2 * mine + at + mine, span]
                    hi = got[4 * mine + at : 4 * mine + at + mine, span]
                    value = (
                        mid
                        + jnp.where(lane < width - 1, pltpu.roll(lo, width - 1, 1), 0.0)
                        + jnp.where(lane > 0, pltpu.roll(hi, 1, 1), 0.0)
                    )
                    sums[plane, pl.ds(h + i, mine, stride=height), :] = value

    def round_rows(c):
        first = c * ROWS
        for plane in range(2):
            for i in range(mine):
                value = sums[plane, i * height + first : i * height + first + ROWS, :]
                gi_ref[i, plane, first : first + ROWS, :] = value.astype(jnp.bfloat16)

    def lay_own(c):
        for plane in range(2):
            lay(0, plane + 1, c)
        for side in range(2):
            lay_halo(0, side, c)
        compute(0, c)

    def finish(c):
        for rel in range(1, n_chan):
            for side in range(2):
                lay_halo(rel, side, c)
            compute(rel, c)

    def forward(plane, c):
        for rel in range(1, n_chan):
            y_copy(n_chan - rel, plane, c).wait_recv()

            @pl.when(jnp.logical_and(plane == 0, below))
            def _():
                halo_copy(rel, 0, c).start()

            @pl.when(jnp.logical_and(plane == 1, above))
            def _():
                halo_copy(rel, 1, c).start()

    blocks = n_space // n_chan
    keep = mine // blocks
    leave[...] = jnp.zeros_like(leave)

    def fill_share(rel):
        for b in range(3):
            for e in range(3):
                top = 2 * e * mine
                share = total[rel, b, top : top + mine, :] + pltpu.roll(
                    total[rel, b, top + mine : top + 2 * mine, :], group - mine, 1
                )
                share = share.astype(jnp.bfloat16)
                at = (3 * b + e) * keep
                for j in range(blocks):
                    leave[rel, j, at : at + keep, :] = share[j * keep : (j + 1) * keep]

    def share_copy(rel, j):
        return pltpu.make_async_remote_copy(
            src_ref=leave.at[rel, j],
            dst_ref=land.at[s],
            send_sem=s_send.at[rel, j],
            recv_sem=s_recv.at[s],
            device_id=(k * blocks + j, place(k, rel, n_chan)),
            device_id_type=pl.DeviceIdType.MESH,
        )

    def each_share(rel, act, own):
        for turn in range(blocks):
            j = lax.rem(turn + s, blocks)
            if rel == 0:
                here = k * blocks + j == s

                @pl.when(jnp.logical_not(here))
                def _():
                    act(share_copy(rel, j))

                if own:

                    @pl.when(here)
                    def _():
                        pltpu.make_async_copy(leave.at[rel, j], land.at[s], s_recv.at[s]).start()

            else:
                act(share_copy(rel, j))

    def send_share(rel):
        fill_share(rel)
        each_share(rel, lambda d: d.start(), True)

    for plane in range(2):
        own_copy(plane).wait()
    forward(edge, 0)
    for c in range(chunks):
        if c < chunks - 1:
            forward(edge, c + 1)
            lay_own(c)
        if c == 0:
            for i in range(4, rounds + 1):
                advance(i)
        if c == chunks - 2:
            lay_own(chunks - 1)
            advance(rounds + 1)
            send_share(0)
        if c:
            finish(c - 1)
            compute_inputs(c - 1)
            if c > 1:
                round_rows(c - 2)
        forward(inner, c)
        for rel in range(1, n_chan):
            for plane in range(2):
                lay(rel, plane + 1, c)
    finish(chunks - 1)
    for rel in range(1, n_chan):
        send_share(rel)
    compute_inputs(chunks - 1)
    for c in range(max(chunks - 2, 0), chunks):
        round_rows(c)

    for i in range(n_space):
        pltpu.make_async_copy(land.at[i], land.at[i], s_recv.at[i]).wait()
    result = land[0].astype(jnp.float32)
    for i in range(1, n_space):
        result += land[i].astype(jnp.float32)
    gf_ref[...] = result

    for rel in range(n_chan):
        each_share(rel, lambda d: d.wait_send(), False)
    for c in range(chunks):
        for rel in range(1, n_chan):
            for plane in range(2):
                y_copy(rel, plane, c).wait_send()
        for rel in range(n_chan):

            @pl.when(below)
            def _():
                halo_copy(rel, 0, c).wait_send()

            @pl.when(above)
            def _():
                halo_copy(rel, 1, c).wait_send()


def fused(n_space, n_chan, inputs, grad_out, filt):
    mine, planes, height, width = inputs.shape
    keep = filt.shape[2] // n_space
    blocks = n_space // n_chan
    share_rows = -(-9 * keep // 16) * 16
    chunks = height // ROWS
    group = 4 * mine
    dma = pltpu.SemaphoreType.DMA
    vmem = pl.BlockSpec(memory_space=pltpu.VMEM)
    rounds = n_space.bit_length() - 1
    hbm = pl.BlockSpec(memory_space=pltpu.HBM)
    grad_inputs, share = pl.pallas_call(
        functools.partial(body, n_space, n_chan),
        out_shape=(
            jax.ShapeDtypeStruct(inputs.shape, jnp.bfloat16),
            jax.ShapeDtypeStruct((share_rows, group), jnp.float32),
        ),
        in_specs=[hbm, hbm, hbm],
        out_specs=(vmem, vmem),
        scratch_shapes=[
            pltpu.VMEM((n_chan, 4, mine, height, width), jnp.bfloat16),
            pltpu.VMEM((n_chan * group, (height + 2) * width), jnp.bfloat16),
            pltpu.VMEM((6 * mine, (height + 2) * width), jnp.bfloat16),
            pltpu.VMEM((mine * ROWS, width), jnp.float32),
            pltpu.VMEM((n_chan, 3, 6 * mine, group), jnp.float32),
            pltpu.VMEM((3, 6 * mine, n_chan * group), jnp.bfloat16),
            pltpu.VMEM(inputs.shape, jnp.bfloat16),
            pltpu.VMEM(filt.shape, jnp.bfloat16),
            pltpu.VMEM((n_chan, 9 * mine, group), jnp.bfloat16),
            pltpu.VMEM((n_chan, 9 * mine, group), jnp.bfloat16),
            pltpu.VMEM((2, mine * height, width), jnp.float32),
            pltpu.VMEM((n_chan, blocks, share_rows, group), jnp.bfloat16),
            pltpu.VMEM((n_space, share_rows, group), jnp.bfloat16),
            dma((2,)),
            dma((2,)),
            dma((n_chan - 1, 2, chunks)),
            dma((n_chan, 2, chunks)),
            dma((n_chan, 4, chunks)),
            dma((n_chan - 1,)),
            dma((n_chan - 1,)),
            dma((n_chan, blocks)),
            dma((n_space,)),
            pltpu.SemaphoreType.REGULAR((rounds + 1,)),
        ],
        compiler_params=pltpu.CompilerParams(has_side_effects=True, collective_id=0, vmem_limit_bytes=24 << 20),
    )(*(pltpu.with_memory_space_constraint(x, pltpu.HBM) for x in (filt, inputs, grad_out)))
    share = share[: 9 * keep].reshape(9, keep, 4, mine)[:, :, 2::-1]
    return grad_inputs, share.transpose(2, 0, 3, 1).reshape(27, mine, keep)


def solution(mesh):
    n_space, n_chan = mesh.shape["space"], mesh.shape["chan"]

    def run(inputs, grad_out, filt):
        mine, planes, height, width = inputs.shape
        fits = (
            planes == 2
            and n_chan > 1
            and width == 128
            and 4 * mine == width
            and grad_out.shape[0] == mine
            and filt.shape[2] == n_chan * mine
            and height % ROWS == 0
            and n_space % n_chan == 0
            and n_space & (n_space - 1) == 0
            and n_space >= 8
            and height // ROWS >= 3
            and filt.shape[2] % n_space == 0
        )
        if fits:
            return fused(n_space, n_chan, inputs, grad_out, filt)
        return local(inputs, grad_out, filt)

    return jax.shard_map(
        run,
        mesh=mesh,
        in_specs=(
            P("chan", "space", None, None),
            P("chan", "space", None, None),
            P(None, "chan", None),
        ),
        out_specs=(P("chan", "space", None, None), P(None, "chan", "space")),
        check_vma=False,
    )
```
